32 devices in a mesh: rep: 4 (over x, y), dp: 8 (over z, core).
Axes of the slice: x: 2, y: 2, z: 4, core: 2. Of those that a mesh axis runs over, the one named last changes fastest.
Arguments:
- g_w_gate: bfloat16 [32, 2, 1536, 4224], P(('rep', 'dp')), parts along dimension 0
- g_w_up: bfloat16 [32, 2, 1536, 4224], P(('rep', 'dp')), parts along dimension 0
- g_w_down: bfloat16 [32, 2, 4224, 1536], P(('rep', 'dp')), parts along dimension 0
- w_gate: bfloat16 [2, 1536, 4224], replicated
- w_up: bfloat16 [2, 1536, 4224], replicated
- w_down: bfloat16 [2, 4224, 1536], replicated
- m_w_gate: float32 [2, 1536, 4224], P(None, 'dp')
- m_w_up: float32 [2, 1536, 4224], P(None, 'dp')
- m_w_down: float32 [2, 4224, 1536], P(None, 'dp')
- v_w_gate: float32 [2, 1536, 4224], P(None, 'dp')
- v_w_up: float32 [2, 1536, 4224], P(None, 'dp')
- v_w_down: float32 [2, 4224, 1536], P(None, 'dp')
Outputs:
- output 1: bfloat16 [8, 1536, 4224], P('rep'), parts along dimension 0
- output 2: bfloat16 [8, 1536, 4224], P('rep'), parts along dimension 0
- output 3: bfloat16 [8, 4224, 1536], P('rep'), parts along dimension 0
- output 4: float32 [8, 1536, 4224], P('rep', 'dp'), parts along dimension 0
- output 5: float32 [8, 1536, 4224], P('rep', 'dp'), parts along dimension 0
- output 6: float32 [8, 4224, 1536], P('rep', 'dp'), parts along dimension 0
- output 7: float32 [8, 1536, 4224], P('rep', 'dp'), parts along dimension 0
- output 8: float32 [8, 1536, 4224], P('rep', 'dp'), parts along dimension 0
- output 9: float32 [8, 4224, 1536], P('rep', 'dp'), parts along dimension 0
There are 4 independent parts. The reference program is written for one: setup_inputs(seed, part) draws one part's arguments, and reference() takes and returns one part's arrays. A program takes and returns all parts, laid end to end along the dimension named above; an argument that names none is the same for every part.
All inputs are finite; a program needn't handle non-finite values.
Results may differ from the reference program's by a relative error of at most 0.022.
Values are sent between devices in bfloat16 or wider.
A program may use at most 2 GiB of HBM per device.

```python
import jax
import jax.numpy as jnp
from jax import lax

DEVICES = 8
D = 1536
FF = 4224
LAYERS = 2
NAMES = ("w_gate", "w_up", "w_down")
SHAPES = {"w_gate": (LAYERS, D, FF), "w_up": (LAYERS, D, FF), "w_down": (LAYERS, FF, D)}


def setup_inputs(seed: int = 0, part: int = 0) -> dict:
    kz, *keys = jax.random.split(jax.random.key(seed), 1 + 5 * len(NAMES))
    loud = 2.0 ** jax.random.uniform(kz, (), jnp.float32, -1.0, 1.0)
    drawn = {}
    for name, key, both in zip(NAMES, keys[:3], keys[3:6], strict=True):
        own = jax.random.normal(jax.random.fold_in(key, part), (DEVICES, *SHAPES[name]), jnp.float32)
        shared = jax.random.normal(jax.random.fold_in(both, part), SHAPES[name], jnp.float32)
        drawn["g_" + name] = (loud * (0.7 * shared / DEVICES + 0.7 * own * DEVICES**-0.5)).astype(jnp.bfloat16)
    for name, key in zip(NAMES, keys[6:9], strict=True):
        drawn[name] = (jax.random.normal(key, SHAPES[name], jnp.float32) * SHAPES[name][1] ** -0.5).astype(jnp.bfloat16)
    for name, key in zip(NAMES, keys[9:12], strict=True):
        drawn["m_" + name] = loud * 0.5 * jax.random.normal(key, SHAPES[name], jnp.float32)
    for name, key in zip(NAMES, keys[12:15], strict=True):
        drawn["v_" + name] = loud * loud * jax.random.uniform(key, SHAPES[name], jnp.float32, 0.5, 1.5)
    return drawn


def adamw(w, m, v, g):
    m = 0.9 * m + 0.1 * g
    v = 0.95 * v + 0.05 * g * g
    step = m * lax.rsqrt(v + 1e-8) + 0.1 * w
    return (w - 0.02 * step).astype(jnp.bfloat16), m, v


def clipped(gradients, sum_of_squares, count):
    factor = jnp.minimum(1.0, 0.5 * lax.rsqrt(sum_of_squares / count + 1e-30))
    return [g * factor for g in gradients]


def reference(g_w_gate, g_w_up, g_w_down, w_gate, w_up, w_down, m_w_gate, m_w_up, m_w_down, v_w_gate, v_w_up, v_w_down):
    def total(terms):
        return lax.scan(lambda so_far, term: (so_far + term.astype(jnp.float32), None), jnp.zeros(terms.shape[1:], jnp.float32), terms)[0]

    gradients = [total(terms).astype(jnp.bfloat16).astype(jnp.float32) for terms in (g_w_gate, g_w_up, g_w_down)]
    gradients = clipped(gradients, sum(jnp.sum(g * g) for g in gradients), sum(g.size for g in gradients))
    new = [
        adamw(w.astype(jnp.float32), m, v, g)
        for w, m, v, g in zip((w_gate, w_up, w_down), (m_w_gate, m_w_up, m_w_down), (v_w_gate, v_w_up, v_w_down), gradients, strict=True)
    ]
    return tuple(one[which] for which in range(3) for one in new)
```

```python
import functools

import jax
import jax.numpy as jnp
from jax import lax
from jax.experimental import pallas as pl
from jax.experimental.pallas import tpu as pltpu
from jax.sharding import PartitionSpec as P

MESH = pl.DeviceIdType.MESH
ANY = pl.BlockSpec(memory_space=pl.ANY)
BF16, F32 = jnp.bfloat16, jnp.float32
PIECES = 3
PER_WEIGHT = 2 * PIECES
PER_BLOCK = 3 * PER_WEIGHT
SLOTS = 3
GROUP = 16


def place():
    rep, dp = lax.axis_index("rep"), lax.axis_index("dp")
    chip, core = dp // 2, lax.rem(dp, 2)
    low = chip < 2
    end = jnp.logical_or(chip == 0, chip == 3)

    def at(near, other=False):
        z = jnp.where(low, near, 3 - near)
        return 2 * z + (1 - core if other else core)

    return rep, dp, end, at


def piece(q):
    return q // PIECES, lax.rem(q, PIECES)


def rows_of(block, height, q, rows):
    return pl.ds(pl.multiple_of(block * height + lax.rem(q, PIECES) * rows, 16), rows)


def remote(src, dst, send, recv, device):
    return pltpu.make_async_remote_copy(src_ref=src, dst_ref=dst, send_sem=send, recv_sem=recv, device_id=device, device_id_type=MESH)


def add_up(rows, ins, out, acc=None):
    @pl.loop(0, rows // GROUP)
    def _(i):
        at = pl.ds(pl.multiple_of(i * GROUP, GROUP), GROUP)
        total = ins[0][at, :].astype(F32)
        for one in ins[1:]:
            total = total + one[at, :].astype(F32)
        rounded = total.astype(BF16)
        out[at, :] = rounded
        if acc is not None:
            g = rounded.astype(F32)
            acc[...] += g * g


def reduce_kernel(heights, *refs):
    terms, m, v = refs[0:3], refs[3:6], refs[6:9]
    g, g_near, m_near, v_near, from_side, from_half, from_core = (refs[9 + 3 * i : 12 + 3 * i] for i in range(7))
    squares = refs[30]
    scratch = refs[31:]
    inward, outward = scratch[0:2], scratch[2:4]
    loads = scratch[4:6]
    acc = scratch[6:8]
    gathered = scratch[8]
    in_send, out_send, load_sem, store_sem, side_sem, half_sem, core_send, core_recv, mv_send, mv_recv, rel_send, rel_recv, sq_send, sq_recv = scratch[9:]
    rep, dp, end, at = place()
    partner = (rep, at(jnp.where(end, 0, 1), True))
    side = (rep, at(jnp.where(end, 1, 0)))
    half = (rep, at(2))
    rows = [h // PIECES for h in heights]
    kind = (0, 0, 1)

    def core_copy(near, w, layer):
        block = at(near, True)
        n = (near * 3 + w) * 2 + layer
        src = terms[w].at[0, layer, pl.ds(pl.multiple_of(block * heights[w], 16), heights[w]), :]
        return remote(src, from_core[w].at[near, layer], core_send.at[n], core_recv.at[n], partner)

    def mv_copies(w, do_send_sem, do_recv_sem, src_pair, device, quarter, base):
        part = heights[w] // 2
        cut = (quarter // 2, pl.ds(pl.multiple_of(lax.rem(quarter, 2) * part, 8), part))
        out = []
        for i, (src, dst) in enumerate(zip(src_pair, (m_near[w], v_near[w]), strict=True)):
            n = base + 2 * w + i
            out.append(remote(src.at[cut], dst.at[cut], do_send_sem.at[n], do_recv_sem.at[n], device))
        return out

    def relay(w, hop):
        peer = (lax.rem(rep + hop, 4), dp)
        return mv_copies(w, rel_send, rel_recv, (m_near[w], v_near[w]), peer, rep, 6 * (hop - 1))

    def load(w, slot, near, q, ins):
        layer, _ = piece(q)
        sources = [terms[w].at[0, layer, rows_of(at(near), heights[w], q, rows[w]), :]]
        sources += [r.at[layer, rows_of(0, heights[w], q, rows[w]), :] for r in (from_core[w].at[near], *ins)]
        copies = [pltpu.make_async_copy(s, loads[kind[w]].at[slot, i], load_sem.at[slot, i]) for i, s in enumerate(sources)]
        for c in copies:
            c.start()
        return copies

    def into(w, slot, n):
        return [loads[kind[w]].at[slot, i] for i in range(n)]

    def wait_core(near, w, q):
        @pl.when(lax.rem(q, PIECES) == 0)
        def _():
            core_copy(near, w, q // PIECES).wait_recv()

    def side_landing(near, w, q, where):
        layer, _ = piece(q)
        return where.at[layer, rows_of(0, heights[w], q, rows[w]), :]

    def send(w, stage, n, slot, sems, where, q, recv, device):
        return remote(stage[kind[w]].at[slot], side_landing(0, w, q, where), sems.at[kind[w], slot], recv.at[n], device)

    def arrived(w, q, where, recv, n):
        ref = side_landing(0, w, q, where)
        remote(ref, ref, in_send.at[0, 0], recv.at[n], side).wait_recv()

    def reuse(w, q, first, stage, sems, where, recv, device):
        @pl.when(jnp.logical_or(q >= SLOTS, jnp.logical_not(first)))
        def _():
            send(w, stage, 0, lax.rem(q, SLOTS), sems, where, q, recv, device).wait_send()

    acc[0][...] = jnp.zeros_like(acc[0])
    acc[1][...] = jnp.zeros_like(acc[1])

    @pl.when(end)
    def _():
        for near in (3, 2, 1, 0):
            for w in range(3):
                for layer in range(2):
                    core_copy(near, w, layer).start()

    @pl.when(jnp.logical_not(end))
    def _():
        for near in (3, 2, 0, 1):
            for w in range(3):
                for layer in range(2):
                    core_copy(near, w, layer).start()
        for w in range(3):
            for c in mv_copies(w, mv_send, mv_recv, (m[w], v[w]), side, rep, 0):
                c.start()

    @pl.when(end)
    def _():
        for phase, near in enumerate((3, 2, 1)):
            for w in range(3):
                fresh = phase == 0 and w in (0, 2)
                for back in (w - 1,) if phase == 0 else ((2,) if phase == 1 and w == 0 else ()):
                    if back >= 0:
                        for c in mv_copies(back, mv_send, mv_recv, (m_near[back], v_near[back]), side, rep, 0):
                            c.wait_recv()
                        for hop in (1, 2, 3):
                            for c in relay(back, hop):
                                c.start()

                @pl.loop(0, PER_WEIGHT)
                def _(q, w=w, phase=phase, near=near, fresh=fresh):
                    slot = lax.rem(q, SLOTS)
                    wait_core(near, w, q)
                    copies = load(w, 0, near, q, ())
                    own = []
                    if phase == 2:
                        wait_core(0, w, q)
                        arrived(w, q, from_side[w].at[0], side_sem, w * PER_WEIGHT + q)
                        own = load(w, 1, 0, q, (from_side[w].at[0],))
                    reuse(w, q, fresh, inward, in_send, from_side[w].at[phase], side_sem, side)
                    for c in copies:
                        c.wait()
                    add_up(rows[w], into(w, 0, 2), inward[kind[w]].at[slot])
                    send(w, inward, phase * PER_BLOCK + w * PER_WEIGHT + q, slot, in_send, from_side[w].at[phase], q, side_sem, side).start()
                    if phase == 2:
                        layer, _ = piece(q)
                        for c in own:
                            c.wait()
                        out = outward[kind[w]].at[slot]
                        add_up(rows[w], into(w, 1, 3), out, acc[kind[w]])
                        store = pltpu.make_async_copy(out, g[w].at[layer, rows_of(0, heights[w], q, rows[w]), :], store_sem)
                        store.start()
                        store.wait()

        for k in range(2):
            w = (0, 2)[k]
            for slot in range(SLOTS):
                send(w, inward, 0, slot, in_send, from_side[w].at[2], 0, side_sem, side).wait_send()
        for w in range(3):

            @pl.loop(0, PER_WEIGHT)
            def _(q, w=w):
                arrived(w, q, g_near[w], side_sem, PER_BLOCK + w * PER_WEIGHT + q)

            for hop in (1, 2, 3):
                for c in relay(w, hop):
                    c.wait_send()
                source = lax.rem(rep + 4 - hop, 4)
                for c in mv_copies(w, rel_send, rel_recv, (m_near[w], v_near[w]), partner, source, 6 * (hop - 1)):
                    c.wait_recv()

    @pl.when(jnp.logical_not(end))
    def _():
        for phase, near in enumerate((3, 2, 1)):
            for w in range(3):
                fresh = phase == 0 and w in (0, 2)
                fresh_out = phase == 1 and w in (0, 2)

                @pl.loop(0, PER_WEIGHT)
                def _(q, w=w, phase=phase, near=near, fresh=fresh, fresh_out=fresh_out):
                    slot = lax.rem(q, SLOTS)
                    layer, _ = piece(q)
                    n = w * PER_WEIGHT + q
                    if phase == 1:
                        wait_core(0, w, q)
                        arrived(w, q, from_half[w].at[0], half_sem, n)
                        own = load(w, 1, 0, q, (from_half[w].at[0],))
                    wait_core(near, w, q)
                    arrived(w, q, from_side[w].at[phase], side_sem, phase * PER_BLOCK + n)
                    if phase < 2:
                        copies = load(w, 0, near, q, (from_side[w].at[phase],))
                        reuse(w, q, fresh, inward, in_send, from_half[w].at[phase], half_sem, half)
                        for c in copies:
                            c.wait()
                        add_up(rows[w], into(w, 0, 3), inward[kind[w]].at[slot])
                        send(w, inward, phase * PER_BLOCK + n, slot, in_send, from_half[w].at[phase], q, half_sem, half).start()
                        if phase == 1:
                            reuse(w, q, fresh_out, outward, out_send, from_side[w].at[0], side_sem, side)
                            for c in own:
                                c.wait()
                            add_up(rows[w], into(w, 1, 3), outward[kind[w]].at[slot])
                            send(w, outward, n, slot, out_send, from_side[w].at[0], q, side_sem, side).start()
                    else:
                        arrived(w, q, from_half[w].at[1], half_sem, PER_BLOCK + n)
                        copies = load(w, 0, near, q, (from_side[w].at[2], from_half[w].at[1]))
                        reuse(w, q, False, outward, out_send, g_near[w], side_sem, side)
                        for c in copies:
                            c.wait()
                        out = outward[kind[w]].at[slot]
                        add_up(rows[w], into(w, 0, 4), out, acc[kind[w]])
                        send(w, outward, PER_BLOCK + n, slot, out_send, g_near[w], q, side_sem, side).start()
                        store = pltpu.make_async_copy(out, g[w].at[layer, rows_of(0, heights[w], q, rows[w]), :], store_sem)
                        store.start()
                        store.wait()

        for k in range(2):
            w = (0, 2)[k]
            for slot in range(SLOTS):
                send(w, inward, 0, slot, in_send, from_half[w].at[1], 0, half_sem, half).wait_send()
                send(w, outward, 0, slot, out_send, g_near[w], 0, side_sem, side).wait_send()
        for w in range(3):
            for c in mv_copies(w, mv_send, mv_recv, (m[w], v[w]), side, rep, 0):
                c.wait_send()

    for near in range(4):
        for w in range(3):
            for layer in range(2):
                core_copy(near, w, layer).wait_send()

    tile = jnp.zeros((GROUP, 128), F32)
    for one in acc:
        for j in range(one.shape[1] // 128):
            tile = tile + one[:, j * 128 : (j + 1) * 128]
    gathered[dp] = tile
    for hop in range(1, 8):
        to = lax.rem(dp + hop, 8)
        remote(gathered.at[dp], gathered.at[dp], sq_send.at[hop - 1], sq_recv.at[hop - 1], (rep, to)).start()
    for hop in range(1, 8):
        source = lax.rem(dp + 8 - hop, 8)
        c = remote(gathered.at[source], gathered.at[source], sq_send.at[hop - 1], sq_recv.at[hop - 1], (rep, lax.rem(dp + hop, 8)))
        c.wait_send()
        c.wait_recv()
    squares[...] = gathered[...]


def gather_kernel(heights, *refs):
    factor, new, w_old, g_near, m_near, v_near = refs[0], *(refs[1 + 3 * i : 4 + 3 * i] for i in range(5))
    whole = refs[16:19]
    scratch = refs[19:]
    g_in, w_in, m_in, v_in, out = (scratch[2 * i : 2 * i + 2] for i in range(5))
    load_sem, store_sem, ici_send, core_send, side_sem, half_sem, core_recv = scratch[10:]
    rep, dp, end, at = place()
    me = jnp.where(end, 0, 1)
    partner = (rep, at(me, True))
    side = (rep, at(1 - me))
    half = (rep, at(2))
    rows = [h // PIECES for h in heights]
    kind = (0, 0, 1)

    def spot(w, near, q, other=False):
        return whole[w].at[q // PIECES, rows_of(at(near, other), heights[w], q, rows[w]), :]

    def own(w, q):
        return new[w].at[q // PIECES, rows_of(0, heights[w], q, rows[w]), :]

    def to_core(w, near, q, src):
        n = near * PER_BLOCK + w * PER_WEIGHT + q
        return remote(src, spot(w, near, q), core_send.at[n], core_recv.at[n], partner)

    def from_core(w, near, q):
        n = near * PER_BLOCK + w * PER_WEIGHT + q
        ref = spot(w, near, q, True)
        remote(ref, ref, core_send.at[n], core_recv.at[n], partner).wait_recv()

    def to_side(w, near, q, which, src):
        n = which * PER_BLOCK + w * PER_WEIGHT + q
        return remote(src, spot(w, near, q), ici_send.at[n], side_sem.at[n], side)

    def to_half(w, near, q, which, src):
        n = which * PER_BLOCK + w * PER_WEIGHT + q
        return remote(src, spot(w, near, q), ici_send.at[2 * PER_BLOCK + n], half_sem.at[n], half)

    def arrived(w, near, q, which, sem):
        ref = spot(w, near, q)
        remote(ref, ref, ici_send.at[0], sem.at[which * PER_BLOCK + w * PER_WEIGHT + q], side).wait_recv()

    def each(body):
        for w in range(3):

            @pl.loop(0, PER_WEIGHT)
            def _(q, w=w):
                body(w, q)

    @pl.when(end)
    def _():
        def first(w, q):
            to_side(w, 0, q, 0, own(w, q)).start()

        each(first)
        each(lambda w, q: to_core(w, 0, q, own(w, q)).start())

        def compute(w, q):
            k = kind[w]
            layer = q // PIECES
            cut = (layer, rows_of(0, heights[w], q, rows[w]))
            sources = (g_near[w].at[cut], w_old[w].at[layer, rows_of(at(1), heights[w], q, rows[w]), :], m_near[w].at[cut], v_near[w].at[cut])
            copies = [pltpu.make_async_copy(s, d[k], load_sem.at[i]) for i, (s, d) in enumerate(zip(sources, (g_in, w_in, m_in, v_in), strict=True))]
            for c in copies:
                c.start()
            for c in copies:
                c.wait()
            f = factor[0, 0]

            @pl.loop(0, rows[w] // GROUP)
            def _(i):
                part = pl.ds(pl.multiple_of(i * GROUP, GROUP), GROUP)
                g = g_in[k][part, :].astype(F32) * f
                old = w_in[k][part, :].astype(F32)
                m = 0.9 * m_in[k][part, :] + 0.1 * g
                v = 0.95 * v_in[k][part, :] + 0.05 * g * g
                out[k][part, :] = (old - 0.02 * (m * lax.rsqrt(v + 1e-8) + 0.1 * old)).astype(BF16)

            store = pltpu.make_async_copy(out[k], spot(w, 1, q), store_sem)
            pass_on = to_core(w, 1, q, out[k])
            store.start()
            pass_on.start()
            store.wait()
            pass_on.wait_send()

        each(compute)
        for which, near in enumerate((2, 3)):

            def hand_on(w, q, which=which, near=near):
                arrived(w, near, q, which, side_sem)
                to_core(w, near, q, spot(w, near, q)).start()

            each(hand_on)

        def finish(w, q):
            to_side(w, 0, q, 0, own(w, q)).wait_send()
            to_core(w, 0, q, own(w, q)).wait_send()
            to_core(w, 2, q, spot(w, 2, q)).wait_send()
            to_core(w, 3, q, spot(w, 3, q)).wait_send()

        each(finish)

    @pl.when(jnp.logical_not(end))
    def _():
        each(lambda w, q: to_half(w, 1, q, 0, own(w, q)).start())
        each(lambda w, q: to_core(w, 1, q, own(w, q)).start())

        def pass_both(w, q):
            arrived(w, 2, q, 0, half_sem)
            to_side(w, 2, q, 0, spot(w, 2, q)).start()
            to_core(w, 2, q, spot(w, 2, q)).start()
            arrived(w, 0, q, 0, side_sem)
            to_half(w, 0, q, 1, spot(w, 0, q)).start()
            to_core(w, 0, q, spot(w, 0, q)).start()

        each(pass_both)

        def pass_far(w, q):
            arrived(w, 3, q, 1, half_sem)
            to_side(w, 3, q, 1, spot(w, 3, q)).start()
            to_core(w, 3, q, spot(w, 3, q)).start()

        each(pass_far)

        def finish(w, q):
            to_half(w, 1, q, 0, own(w, q)).wait_send()
            to_half(w, 0, q, 1, spot(w, 0, q)).wait_send()
            to_side(w, 2, q, 0, spot(w, 2, q)).wait_send()
            to_side(w, 3, q, 1, spot(w, 3, q)).wait_send()
            to_core(w, 1, q, own(w, q)).wait_send()
            for near in (0, 2, 3):
                to_core(w, near, q, spot(w, near, q)).wait_send()

        each(finish)

    def last(w, q):
        for near in range(4):
            from_core(w, near, q)

    each(last)


def adamw(w, m, v, g):
    m = 0.9 * m + 0.1 * g
    v = 0.95 * v + 0.05 * g * g
    step = m * lax.rsqrt(v + 1e-8) + 0.1 * w
    return (w - 0.02 * step).astype(BF16), m, v


def solution(mesh):
    def step(*arrays):
        terms, weights, m, v = (arrays[i : i + 3] for i in (0, 3, 6, 9))
        heights = tuple(one.shape[1] for one in m)
        widths = tuple(one.shape[2] for one in m)
        block = [(2, h, c) for h, c in zip(heights, widths, strict=True)]
        big = [(h // PIECES, c) for h, c in zip(heights[1:], widths[1:], strict=True)]
        like = lambda lead, t: [jax.ShapeDtypeStruct((*lead, *b), t) for b in block]
        dma = pltpu.SemaphoreType.DMA
        outs = pl.pallas_call(
            functools.partial(reduce_kernel, heights),
            out_shape=(
                *like((), BF16), *like((), BF16), *like((), F32), *like((), F32), *like((3,), BF16), *like((2,), BF16), *like((4,), BF16),
                jax.ShapeDtypeStruct((8, GROUP, 128), F32),
            ),
            in_specs=[ANY] * 9,
            out_specs=(*[ANY] * 21, pl.BlockSpec(memory_space=pltpu.VMEM)),
            scratch_shapes=[
                *[pltpu.VMEM((SLOTS, *b), BF16) for b in big],
                *[pltpu.VMEM((SLOTS, *b), BF16) for b in big],
                *[pltpu.VMEM((2, 4, *b), BF16) for b in big],
                *[pltpu.VMEM((GROUP, b[1]), F32) for b in big],
                pltpu.VMEM((8, GROUP, 128), F32),
                dma((2, SLOTS)), dma((2, SLOTS)), dma((2, 4)), dma,
                dma((3 * PER_BLOCK,)), dma((2 * PER_BLOCK,)), dma((24,)), dma((24,)), dma((6,)), dma((6,)), dma((18,)), dma((18,)), dma((7,)), dma((7,)),
            ],
            compiler_params=pltpu.CompilerParams(has_side_effects=True),
            name="reduce",
        )(*terms, *m, *v)
        g, g_near, m_near, v_near = (outs[i : i + 3] for i in (0, 3, 6, 9))
        squares = jnp.sum(outs[21])
        count = 8 * sum(one.size for one in m)
        factor = jnp.minimum(1.0, 0.5 * lax.rsqrt(squares / count + 1e-30))
        me = lax.axis_index("dp")
        own = [lax.dynamic_slice_in_dim(w, me * h, h, 1).astype(F32) for w, h in zip(weights, heights, strict=True)]
        new = [adamw(w, m, v, g.astype(F32) * factor) for w, m, v, g in zip(own, m, v, g, strict=True)]
        whole = pl.pallas_call(
            functools.partial(gather_kernel, heights),
            out_shape=tuple(jax.ShapeDtypeStruct(w.shape, BF16) for w in weights),
            in_specs=[pl.BlockSpec(memory_space=pltpu.SMEM), *[ANY] * 15],
            out_specs=(ANY,) * 3,
            scratch_shapes=[
                *[pltpu.VMEM(b, BF16) for b in big], *[pltpu.VMEM(b, BF16) for b in big],
                *[pltpu.VMEM(b, F32) for b in big], *[pltpu.VMEM(b, F32) for b in big],
                *[pltpu.VMEM(b, BF16) for b in big],
                dma((4,)), dma, dma((4 * PER_BLOCK,)), dma((4 * PER_BLOCK,)), dma((2 * PER_BLOCK,)), dma((2 * PER_BLOCK,)), dma((4 * PER_BLOCK,)),
            ],
            compiler_params=pltpu.CompilerParams(has_side_effects=True),
            name="gather",
        )(factor.reshape(1, 1), *(one[0] for one in new), *weights, *g_near, *m_near, *v_near)
        whole = [lax.dynamic_update_slice_in_dim(w, one[0], me * h, 1) for w, one, h in zip(whole, new, heights, strict=True)]
        return (*whole, *(one[1] for one in new), *(one[2] for one in new))

    all_of, cut = P(None, None, None), P(None, "dp", None)
    return jax.shard_map(
        step,
        mesh=mesh,
        in_specs=(P(("rep", "dp"), None, None, None),) * 3 + (all_of,) * 3 + (cut,) * 6,
        out_specs=(P("rep", None, None),) * 3 + (P("rep", "dp", None),) * 6,
        check_vma=False,
    )
```
